32 devices in a mesh: dp: 8 (over y, x, core), rep: 4 (over z).
Axes of the slice: x: 2, y: 2, z: 4, core: 2. Of those that a mesh axis runs over, the one named last changes fastest.
Arguments:
- student_in: bfloat16 [16384, 320], P(('dp', 'rep')), may hold values from -6 to 6
- target_in: bfloat16 [16384, 320], P(('dp', 'rep')), may hold values from -6 to 6
- timesteps: int32 [64], P(('dp', 'rep')), may hold values from 20 to 999
- student_win: float32 [1280, 320], P('dp'), may hold values from -0.3125 to 0.3125
- student_wout: float32 [640, 320], P('dp'), may hold values from -0.25 to 0.25
- student_wtime: float32 [640, 320], P('dp'), may hold values from -0.25 to 0.25
- student_gain: float32 [320], replicated, may hold values from 0.5 to 1.5
- student_bias: float32 [320], replicated, may hold values from -3 to 3
- target_win: float32 [1280, 320], P('dp'), may hold values from -0.3125 to 0.3125
- target_wout: float32 [640, 320], P('dp'), may hold values from -0.25 to 0.25
- target_wtime: float32 [640, 320], P('dp'), may hold values from -0.25 to 0.25
- target_gain: float32 [320], replicated, may hold values from 0.5 to 1.5
- target_bias: float32 [320], replicated, may hold values from -3 to 3
Outputs:
- grad_win: float32 [1280, 320], P('dp')
- grad_wout: float32 [640, 320], P('dp')
- grad_wtime: float32 [640, 320], P('dp')
- grad_gain: float32 [320], replicated
- grad_bias: float32 [320], replicated
- ema_win: float32 [1280, 320], P('dp')
- ema_wout: float32 [640, 320], P('dp')
- ema_wtime: float32 [640, 320], P('dp')
- ema_gain: float32 [320], replicated
- ema_bias: float32 [320], replicated
The draws below stay inside these ranges and needn't reach their ends.
Inputs may be any that keep to these rules, and one draw needn't show every extreme that they name: `timesteps`: student timestep of each sample; the target is evaluated at 20 steps earlier.
All inputs are finite; a program needn't handle non-finite values.
Results may differ from the reference program's by a relative error of at most 0.004.
The reference program's roundings to bfloat16 on the way (of `time_feat`, `normed_b`, `hidden`, `grad_yb` and `grad_mix`) count: a program that leaves them out, or rounds other values in their place, can miss the bound.
Values may be sent and summed in bfloat16 or wider, within the bound.
A program may use at most 64 MiB of HBM per device.

```python
import math
import jax
import jax.numpy as jnp
from jax import lax

D = 320
FF = 640
TEMB = 640
SKIP = 20
TOK_DEV = 512
SAMPLES = 64
TOKENS = 16384
N_DP = 8


def set_ends(values, key, least, top_value):
    longest = values.shape.index(max(values.shape))
    spots = []
    for shift in (0, 1):
        where = [jax.random.randint(jax.random.fold_in(key, axis), (), 0, length) for axis, length in enumerate(values.shape)]
        where[longest] = (where[longest] + shift) % values.shape[longest]
        spots.append(tuple(where))
    return values.at[spots[0]].set(least).at[spots[1]].set(top_value)


def levels(stream_key, dims, split, least, largest):
    def one(axis_at, shards_of):
        steps = jax.random.uniform(jax.random.fold_in(jax.random.fold_in(stream_key, 6), axis_at), (shards_of,), jnp.float32, least / len(split), largest / len(split))
        return jnp.repeat(jnp.exp(steps), dims[axis_at] // shards_of).reshape((-1,) + (1,) * (len(dims) - axis_at - 1))

    level = one(*split[0])
    for cut in split[1:]:
        level = level * one(*cut)
    return level


def normal_values(own_key, extent, spread, most, shards=(), kind=jnp.bfloat16):
    values = spread * jax.random.normal(own_key, extent, jnp.float32)
    if shards:
        values = values * levels(own_key, extent, shards, -0.22, 0.18)
    return jnp.clip(values, -most, most).astype(kind)


def setup_inputs(seed: int = 0) -> dict:
    keys = jax.random.split(jax.random.key(seed), 14)
    return {
        "student_in": normal_values(keys[0], (TOKENS, D), 1.0, 6.0, ((0, 32),)),
        "target_in": normal_values(keys[1], (TOKENS, D), 1.0, 6.0, ((0, 32),)),
        "timesteps": set_ends(jax.random.randint(keys[2], (SAMPLES,), SKIP, 1000), jax.random.fold_in(keys[2], 1), SKIP, 999).astype(jnp.int32),
        "student_win": normal_values(keys[3], (2 * FF, D), D ** -0.5, 0.3125, ((0, 8),), jnp.float32),
        "student_wout": normal_values(keys[4], (FF, D), FF ** -0.5, 0.25, ((0, 8),), jnp.float32),
        "student_wtime": normal_values(keys[5], (TEMB, D), TEMB ** -0.5, 0.25, ((0, 8),), jnp.float32),
        "student_gain": jnp.clip(1.0 + 0.1 * jax.random.normal(keys[6], (D,), jnp.float32), 0.5, 1.5),
        "student_bias": normal_values(keys[7], (D,), 0.5, 3.0, (), jnp.float32),
        "target_win": normal_values(keys[8], (2 * FF, D), D ** -0.5, 0.3125, ((0, 8),), jnp.float32),
        "target_wout": normal_values(keys[9], (FF, D), FF ** -0.5, 0.25, ((0, 8),), jnp.float32),
        "target_wtime": normal_values(keys[10], (TEMB, D), TEMB ** -0.5, 0.25, ((0, 8),), jnp.float32),
        "target_gain": jnp.clip(1.0 + 0.1 * jax.random.normal(keys[11], (D,), jnp.float32), 0.5, 1.5),
        "target_bias": normal_values(keys[12], (D,), 0.5, 3.0, (), jnp.float32),
    }


ema_decay = 0.95
learn_rate = 0.05

def sinusoid(step_ids, width):
    half_width = width // 2
    frequency = jnp.exp(-math.log(10000.0) * jnp.arange(half_width, dtype=jnp.float32) / half_width)
    angles = step_ids.astype(jnp.float32)[:, None] * frequency[None, :]
    return jnp.concatenate([jnp.cos(angles), jnp.sin(angles)], axis=1)

def gelu_tanh(value):
    inner = 0.7978845608 * (value + 0.044715 * value * value * value)
    return 0.5 * value * (1.0 + jnp.tanh(inner))

def gelu_slope(value):
    tangent = jnp.tanh(0.7978845608 * (value + 0.044715 * value * value * value))
    return 0.5 * (1.0 + tangent) + 0.5 * value * (1.0 - tangent * tangent) * 0.7978845608 * (1.0 + 0.134145 * value * value)

def contract_last(left, right):
    return lax.dot_general(left, right, (((1,), (1,)), ((), ())), preferred_element_type=jnp.float32)

def contract_first(left, right):
    return lax.dot_general(left, right, (((0,), (0,)), ((), ())), preferred_element_type=jnp.float32)

def forward(tok_rows, step_ids, w_in, w_out, w_time, gain, bias):
    time_feat = jax.nn.silu(sinusoid(step_ids, w_time.shape[0])).astype(jnp.bfloat16)
    embedding = jnp.dot(time_feat, w_time, preferred_element_type=jnp.float32)
    samples = step_ids.shape[0]
    width = tok_rows.shape[1]
    summed = tok_rows.astype(jnp.float32).reshape(samples, -1, width) + embedding[:, None, :]
    summed = summed.reshape(-1, width)
    center = summed - lax.optimization_barrier(jnp.mean(summed, axis=1, keepdims=True))
    inv_std = lax.rsqrt(lax.optimization_barrier(jnp.mean(center * center, axis=1, keepdims=True)) + 1e-05)
    normed = center * inv_std
    normed_b = (normed * gain + bias).astype(jnp.bfloat16)
    mixed = contract_last(normed_b, w_in)
    hidden_count = w_out.shape[0]
    gate_part = mixed[:, :hidden_count]
    up_part = mixed[:, hidden_count:]
    gelu_gate = gelu_tanh(gate_part)
    hidden = (gelu_gate * up_part).astype(jnp.bfloat16)
    output = summed + jnp.dot(hidden, w_out, preferred_element_type=jnp.float32)
    return (output, (time_feat, normed, inv_std, normed_b, gate_part, up_part, gelu_gate, hidden))

def backward(grad_y, saved, w_in, w_out, gain):
    time_feat, normed, inv_std, normed_b, gate_part, up_part, gelu_gate, hidden = saved
    grad_yb = grad_y.astype(jnp.bfloat16)
    grad_h = contract_last(grad_yb, w_out)
    grad_mix = jnp.concatenate([grad_h * up_part * gelu_slope(gate_part), grad_h * gelu_gate], axis=1).astype(jnp.bfloat16)
    grad_z = jnp.dot(grad_mix, w_in, preferred_element_type=jnp.float32)
    grad_gain = lax.optimization_barrier(jnp.sum(grad_z * normed, axis=0))
    grad_bias = lax.optimization_barrier(jnp.sum(grad_z, axis=0))
    grad_n = grad_z * gain
    grad_s = grad_y + inv_std * (grad_n - lax.optimization_barrier(jnp.mean(grad_n, axis=1, keepdims=True)) - normed * lax.optimization_barrier(jnp.mean(grad_n * normed, axis=1, keepdims=True)))
    samples = time_feat.shape[0]
    grad_emb = lax.optimization_barrier(jnp.sum(grad_s.reshape(samples, -1, grad_s.shape[1]), axis=1))
    grad_time = lax.dot_general(time_feat.astype(jnp.float32), grad_emb, (((0,), (0,)), ((), ())), precision=lax.Precision.HIGHEST, preferred_element_type=jnp.float32)
    return (grad_yb, grad_mix, grad_gain, grad_bias, grad_time)

def reference(student_in, target_in, timesteps, student_win, student_wout, student_wtime, student_gain, student_bias, target_win, target_wout, target_wtime, target_gain, target_bias):
    s_in = student_win.astype(jnp.bfloat16)
    s_out = student_wout.astype(jnp.bfloat16)
    s_time = student_wtime.astype(jnp.bfloat16)
    t_in = target_win.astype(jnp.bfloat16)
    t_out = target_wout.astype(jnp.bfloat16)
    t_time = target_wtime.astype(jnp.bfloat16)
    width = student_in.shape[1]
    student_blocks = student_in.reshape(N_DP, -1, width)
    target_blocks = target_in.reshape(N_DP, -1, width)
    step_blocks = timesteps.reshape(N_DP, -1)

    def one_block(carry, block):
        s_rows, t_rows, step_ids = block
        student_out, saved = forward(s_rows, step_ids, s_in, s_out, s_time, student_gain, student_bias)
        target_out, unused = forward(t_rows, step_ids - SKIP, t_in, t_out, t_time, target_gain, target_bias)
        grad_y = (student_out - target_out) / TOK_DEV
        grad_yb, grad_mix, grad_gain, grad_bias, grad_time = backward(grad_y, saved, s_in, s_out, student_gain)
        grad_in = contract_first(grad_mix, saved[3])
        grad_out = contract_first(saved[7], grad_yb)
        totals = (carry[0] + grad_in, carry[1] + grad_out, carry[2] + grad_time, carry[3] + grad_gain, carry[4] + grad_bias)
        return (totals, None)
    start = (jnp.zeros(student_win.shape, jnp.float32), jnp.zeros(student_wout.shape, jnp.float32), jnp.zeros(student_wtime.shape, jnp.float32), jnp.zeros(student_gain.shape, jnp.float32), jnp.zeros(student_bias.shape, jnp.float32))
    totals, unused = lax.scan(one_block, start, (student_blocks, target_blocks, step_blocks))
    grad_win, grad_wout, grad_wtime, grad_gain, grad_bias = totals

    def average(target_p, student_p, grad_p):
        return ema_decay * target_p + (1.0 - ema_decay) * (student_p - learn_rate * grad_p)
    return (grad_win, grad_wout, grad_wtime, grad_gain, grad_bias, average(target_win, student_win, grad_win), average(target_wout, student_wout, grad_wout), average(target_wtime, student_wtime, grad_wtime), average(target_gain, student_gain, grad_gain), average(target_bias, student_bias, grad_bias))
```

```python
import functools
import math

import jax
import jax.numpy as jnp
from jax import lax
from jax.experimental import pallas as pl
from jax.experimental.pallas import tpu as pltpu
from jax.sharding import PartitionSpec as P

MESH = pl.DeviceIdType.MESH
SUB = 8

SKIP = 20


ema_decay = 0.95
learn_rate = 0.05


def sinusoid(step_ids, width):
    half_width = width // 2
    frequency = jnp.exp(-math.log(10000.0) * jnp.arange(half_width, dtype=jnp.float32) / half_width)
    angles = step_ids.astype(jnp.float32)[:, None] * frequency[None, :]
    return jnp.concatenate([jnp.cos(angles), jnp.sin(angles)], axis=1)


def gelu_tanh(value):
    inner = 0.7978845608 * (value + 0.044715 * value * value * value)
    return 0.5 * value * (1.0 + jnp.tanh(inner))


def gelu_slope(value):
    tangent = jnp.tanh(0.7978845608 * (value + 0.044715 * value * value * value))
    return 0.5 * (1.0 + tangent) + 0.5 * value * (1.0 - tangent * tangent) * 0.7978845608 * (
        1.0 + 0.134145 * value * value
    )


def contract_last(left, right):
    return lax.dot_general(
        left, right, (((1,), (1,)), ((), ())), preferred_element_type=jnp.float32
    )


def contract_first(left, right):
    return lax.dot_general(
        left, right, (((0,), (0,)), ((), ())), preferred_element_type=jnp.float32
    )


def forward(tok_rows, step_ids, w_in, w_out, w_time, gain, bias):
    time_feat = jax.nn.silu(sinusoid(step_ids, w_time.shape[0])).astype(jnp.bfloat16)
    embedding = jnp.dot(time_feat, w_time, preferred_element_type=jnp.float32)
    samples = step_ids.shape[0]
    width = tok_rows.shape[1]
    summed = tok_rows.astype(jnp.float32).reshape(samples, -1, width) + embedding[:, None, :]
    summed = summed.reshape(-1, width)
    center = summed - jnp.mean(summed, axis=1, keepdims=True)
    inv_std = lax.rsqrt(jnp.mean(center * center, axis=1, keepdims=True) + 1e-05)
    normed = center * inv_std
    normed_b = (normed * gain + bias).astype(jnp.bfloat16)
    mixed = contract_last(normed_b, w_in)
    hidden_count = w_out.shape[0]
    gate_part = mixed[:, :hidden_count]
    up_part = mixed[:, hidden_count:]
    gelu_gate = gelu_tanh(gate_part)
    hidden = (gelu_gate * up_part).astype(jnp.bfloat16)
    output = summed + jnp.dot(hidden, w_out, preferred_element_type=jnp.float32)
    return (output, (time_feat, normed, inv_std, normed_b, gate_part, up_part, gelu_gate, hidden))


def backward(grad_y, saved, w_in, w_out, gain):
    time_feat, normed, inv_std, normed_b, gate_part, up_part, gelu_gate, hidden = saved
    grad_yb = grad_y.astype(jnp.bfloat16)
    grad_h = contract_last(grad_yb, w_out)
    grad_mix = jnp.concatenate(
        [grad_h * up_part * gelu_slope(gate_part), grad_h * gelu_gate], axis=1
    ).astype(jnp.bfloat16)
    grad_z = jnp.dot(grad_mix, w_in, preferred_element_type=jnp.float32)
    grad_gain = jnp.sum(grad_z * normed, axis=0)
    grad_bias = jnp.sum(grad_z, axis=0)
    grad_n = grad_z * gain
    grad_s = grad_y + inv_std * (
        grad_n
        - jnp.mean(grad_n, axis=1, keepdims=True)
        - normed * jnp.mean(grad_n * normed, axis=1, keepdims=True)
    )
    samples = time_feat.shape[0]
    grad_emb = jnp.sum(grad_s.reshape(samples, -1, grad_s.shape[1]), axis=1)
    grad_time = lax.dot_general(
        time_feat.astype(jnp.float32),
        grad_emb,
        (((0,), (0,)), ((), ())),
        precision=lax.Precision.HIGHEST,
        preferred_element_type=jnp.float32,
    )
    return (grad_yb, grad_mix, grad_gain, grad_bias, grad_time)


def fetch(piece_in, piece_out, piece_time):
    return (
        lax.all_gather(piece_in, "dp", axis=0, tiled=True),
        lax.all_gather(piece_out, "dp", axis=0, tiled=True),
        lax.all_gather(piece_time, "dp", axis=0, tiled=True),
    )


def per_device(
    student_in,
    target_in,
    timesteps,
    student_win,
    student_wout,
    student_wtime,
    student_gain,
    student_bias,
    target_win,
    target_wout,
    target_wtime,
    target_gain,
    target_bias,
):
    s_in, s_out, s_time = fetch(
        student_win.astype(jnp.bfloat16),
        student_wout.astype(jnp.bfloat16),
        student_wtime.astype(jnp.bfloat16),
    )
    student_out, saved = forward(
        student_in, timesteps, s_in, s_out, s_time, student_gain, student_bias
    )
    t_in, t_out, t_time = fetch(
        target_win.astype(jnp.bfloat16),
        target_wout.astype(jnp.bfloat16),
        target_wtime.astype(jnp.bfloat16),
    )
    target_out, unused = forward(
        target_in, timesteps - SKIP, t_in, t_out, t_time, target_gain, target_bias
    )
    grad_y = (student_out - target_out) / student_in.shape[0]
    back_in, back_out = (
        lax.all_gather(student_win.astype(jnp.bfloat16), "dp", axis=0, tiled=True),
        lax.all_gather(student_wout.astype(jnp.bfloat16), "dp", axis=0, tiled=True),
    )
    grad_yb, grad_mix, grad_gain, grad_bias, grad_time = backward(
        grad_y, saved, back_in, back_out, student_gain
    )
    normed_b = saved[3]
    hidden = saved[7]
    part = grad_mix
    shard_in = lax.psum_scatter(
        contract_first(part, normed_b), "dp", scatter_dimension=0, tiled=True
    )
    part = hidden
    shard_out = lax.psum_scatter(
        contract_first(part, grad_yb), "dp", scatter_dimension=0, tiled=True
    )
    shard_time = lax.psum_scatter(grad_time, "dp", scatter_dimension=0, tiled=True)
    shard_in, shard_out, shard_time = lax.psum((shard_in, shard_out, shard_time), "rep")
    total_gain, total_bias = lax.psum((grad_gain, grad_bias), ("dp", "rep"))

    def average(target_p, student_p, grad_p):
        return ema_decay * target_p + (1.0 - ema_decay) * (student_p - learn_rate * grad_p)

    return (
        shard_in,
        shard_out,
        shard_time,
        total_gain,
        total_bias,
        average(target_win, student_win, shard_in),
        average(target_wout, student_wout, shard_out),
        average(target_wtime, student_wtime, shard_time),
        average(target_gain, student_gain, total_gain),
        average(target_bias, student_bias, total_bias),
    )


def time_features(step_ids, width):
    return jax.nn.silu(sinusoid(step_ids, width)).astype(jnp.bfloat16)


def fused_kernel(
    n_rep, n_sam,
    x_s, x_t, tf, sw, so, st, sg, sb, tw, to, tt, tg, tb,
    gw_o, go_o, gt_o, gg_o, gb_o, ew_o, eo_o, et_o, eg_o, eb_o,
    ws_all, os_all, wt_all, ot_all,
    tf_all, e_part, e_in, small, small_rep,
    normed_v, inv_v, nb_v, hid_v, a_v, b_v, y_v, nbt_v, gyb_v, gma_v, gmb_v,
    g_win, g_out, gb_win, gb_out, r1_win, r1_out, s2_win, s2_out, r2_win, r2_out,
    p_v, pb_v, r3_v, fin_v,
    g_send, g_recv, tf_send, tf_recv, e_send, e_recv, sm_send, sm_recv,
    r1_send, r1_recv, r2_send, r2_recv, r3_send, r3_recv, r4_send, r4_recv, rs_send, rs_recv,
):
    f32, bf16 = jnp.float32, jnp.bfloat16
    me, rep = lax.axis_index("dp"), lax.axis_index("rep")
    core, col, row = lax.rem(me, 2), lax.rem(lax.div(me, 2), 2), lax.div(me, 4)
    rows_in, rows_out, rows_time = sw.shape[0], so.shape[0], st.shape[0]
    tokens = x_s.shape[0]
    per = tokens // n_sam
    ff = os_all.shape[0]

    def peer(t):
        flip = lambda b, on: 1 - b if on else b
        return flip(row, t & 4) * 4 + flip(col, t & 2) * 2 + flip(core, t & 1)

    def dp_id(t):
        return {"dp": peer(t)}

    def rep_at(j):
        return lax.rem(rep + j, n_rep)

    sends = []

    def send(src, dst, s_sem, r_sem, where):
        copy = pltpu.make_async_remote_copy(
            src_ref=src, dst_ref=dst, send_sem=s_sem, recv_sem=r_sem,
            device_id=where, device_id_type=MESH,
        )
        copy.start()
        sends.append(copy)

    def arrive(dst, s_sem, r_sem):
        pltpu.make_async_remote_copy(
            src_ref=dst, dst_ref=dst, send_sem=s_sem, recv_sem=r_sem,
            device_id=dp_id(1), device_id_type=MESH,
        ).wait_recv()

    def block(ref, owner, count):
        return ref.at[pl.ds(pl.multiple_of(owner * count, 16), count)]

    bufs = (ws_all, os_all, wt_all, ot_all)
    counts = (rows_in, rows_out, rows_in, rows_out)
    firsts = (2, 4, 4, 2)
    for buf, own, count in zip(bufs, (sw, so, tw, to), counts):
        buf[pl.ds(pl.multiple_of(me * count, 16), count), :] = own[...].astype(bf16)
    tf_all[pl.ds(me, 1)] = tf[pl.ds(me, 1)]

    barrier = pltpu.get_barrier_semaphore()
    for t in range(1, 8):
        pl.semaphore_signal(barrier, inc=1, device_id=dp_id(t), device_id_type=MESH)
    for j in range(1, n_rep):
        pl.semaphore_signal(barrier, inc=1, device_id={"rep": rep_at(j)}, device_id_type=MESH)
    pl.semaphore_wait(barrier, 7 + n_rep - 1)

    def push(seg, orel, t, k):
        part = block(bufs[seg], peer(orel), counts[seg])
        send(part, part, g_send.at[seg * 8 + k], g_recv.at[seg * 8 + (orel ^ t)], dp_id(t))

    def landed(seg, orel):
        arrive(block(bufs[seg], peer(orel), counts[seg]), g_send.at[0], g_recv.at[seg * 8 + orel])

    def open_gather(seg):
        push(seg, 0, firsts[seg], 0)
        push(seg, 0, 6 - firsts[seg], 1)
        push(seg, 0, 1, 2)

    def relay_near(seg):
        first, second = firsts[seg], 6 - firsts[seg]
        landed(seg, first)
        push(seg, first, second, 3)
        push(seg, first, 1, 4)
        landed(seg, second)
        push(seg, second, 1, 5)

    def relay_far(seg):
        landed(seg, 6)
        push(seg, 6, 1, 6)

    def close_gather(seg):
        for orel in (1, 3, 5, 7):
            landed(seg, orel)

    for t in range(1, 8):
        send(tf.at[peer(t)], tf_all.at[me], tf_send.at[t], tf_recv.at[t], dp_id(t))
    open_gather(0)
    for t in range(1, 8):
        arrive(tf_all.at[peer(t)], tf_send.at[t], tf_recv.at[t])
    feats = tf_all[...].reshape(8 * SUB, rows_time).astype(bf16)
    part_s = jnp.dot(feats, st[...].astype(bf16), preferred_element_type=f32)
    part_t = jnp.dot(feats, tt[...].astype(bf16), preferred_element_type=f32)
    line = lax.rem(lax.broadcasted_iota(jnp.int32, part_s.shape, 0), SUB)
    e_part[...] = jnp.where(line < n_sam, part_s, part_t).reshape(e_part.shape)
    e_in[pl.ds(me, 1)] = e_part[pl.ds(me, 1)]
    for t in range(1, 8):
        send(e_part.at[peer(t)], e_in.at[me], e_send.at[t], e_recv.at[t], dp_id(t))
    open_gather(1)
    open_gather(2)
    open_gather(3)
    relay_near(0)
    for t in range(1, 8):
        arrive(e_in.at[peer(t)], e_send.at[t], e_recv.at[t])
    emb = e_in[0]
    for k in range(1, 8):
        emb = emb + e_in[k]

    def normalise(x_ref, k, shift, gain, bias):
        summed = x_ref[pl.ds(k * per, per), :].astype(f32) + shift
        center = summed - jnp.mean(summed, axis=1, keepdims=True)
        inv = lax.rsqrt(jnp.mean(center * center, axis=1, keepdims=True) + 1e-05)
        normed = center * inv
        return summed, inv, normed, (normed * gain + bias).astype(bf16)

    for k in range(n_sam):
        at = pl.ds(k * per, per)
        summed, inv, normed, nb = normalise(x_s, k, emb[k : k + 1], sg[...], sb[...])
        y_v[at, :], normed_v[at, :], nb_v[at, :] = summed, normed, nb
        inv_v[at, :] = inv
    relay_far(0)
    relay_near(1)
    for k in range(n_sam):
        at = pl.ds(k * per, per)
        summed, inv, normed, nb = normalise(x_t, k, emb[n_sam + k : n_sam + k + 1], tg[...], tb[...])
        y_v[at, :], nbt_v[at, :] = y_v[at, :] - summed, nb
    close_gather(0)
    relay_far(1)

    for k in range(n_sam):
        at = pl.ds(k * per, per)
        gate = contract_last(nb_v[at, :], ws_all[:ff, :])
        up = contract_last(nb_v[at, :], ws_all[ff:, :])
        tangent = jnp.tanh(0.7978845608 * (gate + 0.044715 * gate * gate * gate))
        half = 0.5 * (1.0 + tangent)
        act = gate * half
        slope = half + 0.5 * gate * (1.0 - tangent * tangent) * 0.7978845608 * (
            1.0 + 0.134145 * gate * gate
        )
        a_v[at, :], b_v[at, :] = up * slope, act
        hid_v[at, :] = (act * up).astype(bf16)
        if k == 0:
            relay_near(2)
            close_gather(1)
    relay_far(2)
    relay_near(3)
    for k in range(n_sam):
        at = pl.ds(k * per, per)
        y_v[at, :] = y_v[at, :] + jnp.dot(hid_v[at, :], os_all[...], preferred_element_type=f32)
    close_gather(2)
    relay_far(3)

    for k in range(n_sam):
        at = pl.ds(k * per, per)
        gate = contract_last(nbt_v[at, :], wt_all[:ff, :])
        up = contract_last(nbt_v[at, :], wt_all[ff:, :])
        hid = (gelu_tanh(gate) * up).astype(bf16)
        if k == 0:
            close_gather(3)
        gy = (y_v[at, :] - jnp.dot(hid, ot_all[...], preferred_element_type=f32)) * (1.0 / tokens)
        y_v[at, :], gyb_v[at, :] = gy, gy.astype(bf16)

    total_out = contract_first(hid_v[...], gyb_v[...])
    g_out[...], gb_out[...] = total_out, total_out.astype(bf16)

    def to_core(src, dst, count, q, k):
        send(block(src, 2 * q + 1 - core, count), dst.at[q], r1_send.at[k], r1_recv.at[k], dp_id(1))

    for q in range(4):
        to_core(gb_out, r1_out, rows_out, q, q)

    grad_gain = jnp.zeros((1, x_s.shape[1]), f32)
    grad_bias = grad_gain
    embs = []
    for k in range(n_sam):
        at = pl.ds(k * per, per)
        gh = contract_last(gyb_v[at, :], os_all[...])
        gma, gmb = (gh * a_v[at, :]).astype(bf16), (gh * b_v[at, :]).astype(bf16)
        gma_v[at, :], gmb_v[at, :] = gma, gmb
        gz = jnp.dot(gma, ws_all[:ff, :], preferred_element_type=f32) + jnp.dot(
            gmb, ws_all[ff:, :], preferred_element_type=f32
        )
        normed = normed_v[at, :]
        grad_gain = grad_gain + jnp.sum(gz * normed, axis=0, keepdims=True)
        grad_bias = grad_bias + jnp.sum(gz, axis=0, keepdims=True)
        gn = gz * sg[...]
        gs = y_v[at, :] + inv_v[at, :] * (
            gn
            - jnp.mean(gn, axis=1, keepdims=True)
            - normed * jnp.mean(gn * normed, axis=1, keepdims=True)
        )
        embs.append(jnp.sum(gs, axis=0, keepdims=True))
    fill = jnp.zeros((SUB - n_sam - 2, x_s.shape[1]), f32)
    small[pl.ds(me, 1)] = jnp.concatenate(embs + [grad_gain, grad_bias, fill], axis=0)[None]

    for h, gm in enumerate((gma_v, gmb_v)):
        total = contract_first(gm[...], nb_v[...])
        at = pl.ds(h * ff, ff)
        g_win[at, :], gb_win[at, :] = total, total.astype(bf16)
        for q in (2 * h, 2 * h + 1):
            to_core(gb_win, r1_win, rows_in, q, 4 + q)
        if h == 0:
            for t in range(1, 8):
                send(small.at[me], small.at[me], sm_send.at[t], sm_recv.at[t], dp_id(t))

    def pair(g, r1, owner_rel, count):
        owner = peer(owner_rel)
        own = g[pl.ds(pl.multiple_of(owner * count, 16), count), :]
        return own + r1[lax.div(owner, 2)].astype(f32)

    for g, r1, s2, r2, count, base in (
        (g_out, r1_out, s2_out, r2_out, rows_out, 0),
        (g_win, r1_win, s2_win, r2_win, rows_in, 4),
    ):
        for q in range(4):
            arrive(r1.at[q], r1_send.at[base + q], r1_recv.at[base + q])
        for k in (3, 1, 2):
            s2[k] = pair(g, r1, 2 * k, count).astype(bf16)
            send(s2.at[k], r2.at[k], r2_send.at[base + k], r2_recv.at[base + k], dp_id(2 * k))

    for t in range(1, 8):
        arrive(small.at[peer(t)], sm_send.at[t], sm_recv.at[t])
    feats = tf_all[...].reshape(8 * SUB, rows_time)
    line = lax.rem(lax.broadcasted_iota(jnp.int32, feats.shape, 0), SUB)
    feats = jnp.where(line < n_sam, feats, 0.0)
    p_v[pl.ds(rows_in + rows_out, rows_time), :] = lax.dot_general(
        feats,
        small[...].reshape(8 * SUB, x_s.shape[1]),
        (((0,), (0,)), ((), ())),
        precision=lax.Precision.HIGHEST,
        preferred_element_type=f32,
    )
    sums = small[0]
    for k in range(1, 8):
        sums = sums + small[k]
    small_rep[pl.ds(rep, 1)] = sums[None]
    for j in range(1, n_rep):
        send(small_rep.at[rep], small_rep.at[rep], rs_send.at[j], rs_recv.at[j], {"rep": rep_at(j)})

    for g, r1, r2, count, base, start in (
        (g_out, r1_out, r2_out, rows_out, 0, rows_in),
        (g_win, r1_win, r2_win, rows_in, 4, 0),
    ):
        total = pair(g, r1, 0, count)
        for k in (1, 2, 3):
            arrive(r2.at[k], r2_send.at[base + k], r2_recv.at[base + k])
            total = total + r2[k].astype(f32)
        p_v[pl.ds(start, count), :] = total
    pb_v[...] = p_v[...].astype(bf16)

    share = p_v.shape[0] // n_rep
    for j in range(1, n_rep):
        send(block(pb_v, rep_at(j), share), r3_v.at[j], r3_send.at[j], r3_recv.at[j], {"rep": rep_at(j)})
    mine = pl.ds(pl.multiple_of(rep * share, 16), share)
    total = p_v[mine, :]
    for j in range(1, n_rep):
        arrive(r3_v.at[j], r3_send.at[j], r3_recv.at[j])
        total = total + r3_v[j].astype(f32)
    fin_v[mine, :] = total
    for j in range(1, n_rep):
        part = block(fin_v, rep, share)
        send(part, part, r4_send.at[j], r4_recv.at[j], {"rep": rep_at(j)})

    for j in range(1, n_rep):
        arrive(small_rep.at[rep_at(n_rep - j)], rs_send.at[j], rs_recv.at[j])
    sums = small_rep[0]
    for j in range(1, n_rep):
        sums = sums + small_rep[j]

    def average(target_p, student_p, grad_p):
        return ema_decay * target_p + (1.0 - ema_decay) * (student_p - learn_rate * grad_p)

    gg, gb = sums[n_sam : n_sam + 1], sums[n_sam + 1 : n_sam + 2]
    gg_o[...], gb_o[...] = gg, gb
    eg_o[...] = average(tg[...], sg[...], gg)
    eb_o[...] = average(tb[...], sb[...], gb)
    for j in range(1, n_rep):
        arrive(block(fin_v, rep_at(n_rep - j), share), r4_send.at[j], r4_recv.at[j])
    start = 0
    for g_o, e_o, student, target in (
        (gw_o, ew_o, sw, tw), (go_o, eo_o, so, to), (gt_o, et_o, st, tt),
    ):
        grad = fin_v[pl.ds(start, g_o.shape[0]), :]
        g_o[...] = grad
        e_o[...] = average(target[...], student[...], grad)
        start += g_o.shape[0]
    for copy in sends:
        copy.wait_send()


def fused_device(n_dp, n_rep, *args):
    (student_in, target_in, timesteps, sw, so, st, sg, sb, tw, to, tt, tg, tb) = args
    f32, bf16 = jnp.float32, jnp.bfloat16
    tokens, width = student_in.shape
    n_sam = timesteps.shape[0]
    rows_in, rows_out, rows_time = sw.shape[0], so.shape[0], st.shape[0]
    ff = rows_out * n_dp
    both = jnp.concatenate([timesteps, timesteps - SKIP])
    feats = time_features(both, rows_time * n_dp).astype(f32)
    feats = jnp.pad(feats, ((0, SUB - 2 * n_sam), (0, 0)))
    feats = feats.reshape(SUB, n_dp, rows_time).transpose(1, 0, 2)
    rows_all = rows_in + rows_out + rows_time
    vm = pltpu.VMEM
    dma = pltpu.SemaphoreType.DMA
    scratch = [
        vm((n_dp * rows_in, width), bf16), vm((ff, width), bf16),
        vm((n_dp * rows_in, width), bf16), vm((ff, width), bf16),
        vm((n_dp, SUB, rows_time), f32), vm((n_dp, SUB, width), f32), vm((n_dp, SUB, width), f32),
        vm((n_dp, SUB, width), f32), vm((n_rep, SUB, width), f32),
        vm((tokens, width), f32), vm((tokens, 1), f32), vm((tokens, width), bf16),
        vm((tokens, ff), bf16), vm((tokens, ff), f32), vm((tokens, ff), f32),
        vm((tokens, width), f32), vm((tokens, width), bf16), vm((tokens, width), bf16),
        vm((tokens, ff), bf16), vm((tokens, ff), bf16),
        vm((n_dp * rows_in, width), f32), vm((ff, width), f32),
        vm((n_dp * rows_in, width), bf16), vm((ff, width), bf16),
        vm((4, rows_in, width), bf16), vm((4, rows_out, width), bf16),
        vm((4, rows_in, width), bf16), vm((4, rows_out, width), bf16),
        vm((4, rows_in, width), bf16), vm((4, rows_out, width), bf16),
        vm((rows_all, width), f32), vm((rows_all, width), bf16),
        vm((n_rep, rows_all // n_rep, width), bf16), vm((rows_all, width), f32),
        dma((32,)), dma((32,)), dma((8,)), dma((8,)), dma((8,)), dma((8,)), dma((8,)), dma((8,)),
        dma((8,)), dma((8,)), dma((8,)), dma((8,)),
        dma((n_rep,)), dma((n_rep,)), dma((n_rep,)), dma((n_rep,)), dma((n_rep,)), dma((n_rep,)),
    ]
    line = lambda v: v.reshape(1, width)
    big = [jax.ShapeDtypeStruct(w.shape, f32) for w in (sw, so, st)]
    flat = [jax.ShapeDtypeStruct((1, width), f32)] * 2
    outs = pl.pallas_call(
        functools.partial(fused_kernel, n_rep, n_sam),
        out_shape=(*big, *flat, *big, *flat),
        in_specs=[pl.BlockSpec(memory_space=vm)] * 13,
        out_specs=[pl.BlockSpec(memory_space=vm)] * 10,
        scratch_shapes=scratch,
        compiler_params=pltpu.CompilerParams(
            collective_id=0, has_side_effects=True, vmem_limit_bytes=60 * 1024 * 1024
        ),
        name="distill_step",
    )(student_in, target_in, feats, sw, so, st, line(sg), line(sb), tw, to, tt, line(tg), line(tb))
    return tuple(o.reshape(width) if o.shape[0] == 1 else o for o in outs)


def fits_fused(n_dp, n_rep, args):
    tokens, samples = args[0].shape[0], args[2].shape[0]
    n_dev = n_dp * n_rep
    rows = [args[i].shape[0] for i in (3, 4, 5)]
    return (
        n_dp == 8
        and n_rep > 1
        and samples % n_dev == 0
        and 2 * (samples // n_dev) + 0 <= SUB
        and samples // n_dev + 2 <= SUB
        and tokens % samples == 0
        and (tokens // samples) % 16 == 0
        and all(r % (16 * n_dp) == 0 for r in rows)
        and (sum(rows) // n_dp) % (16 * n_rep) == 0
        and rows[0] == 2 * rows[1]
    )


def solution(mesh):
    in_specs = (
        P(("dp", "rep"), None),
        P(("dp", "rep"), None),
        P(("dp", "rep")),
        P("dp", None),
        P("dp", None),
        P("dp", None),
        P(),
        P(),
        P("dp", None),
        P("dp", None),
        P("dp", None),
        P(),
        P(),
    )
    out_specs = (
        P("dp", None),
        P("dp", None),
        P("dp", None),
        P(),
        P(),
        P("dp", None),
        P("dp", None),
        P("dp", None),
        P(),
        P(),
    )
    n_dp, n_rep = mesh.shape["dp"], mesh.shape["rep"]

    def step(*args):
        fused = fits_fused(n_dp, n_rep, args)
        body = functools.partial(fused_device, n_dp, n_rep) if fused else per_device
        return jax.shard_map(
            body, mesh=mesh, in_specs=in_specs, out_specs=out_specs, check_vma=False
        )(*args)

    return step
```

```python
import functools
import math

import jax
import jax.numpy as jnp
from jax import lax
from jax.experimental import pallas as pl
from jax.experimental.pallas import tpu as pltpu
from jax.sharding import PartitionSpec as P

MESH = pl.DeviceIdType.MESH
SUB = 8

SKIP = 20


ema_decay = 0.95
learn_rate = 0.05


def sinusoid(step_ids, width):
    half_width = width // 2
    frequency = jnp.exp(-math.log(10000.0) * jnp.arange(half_width, dtype=jnp.float32) / half_width)
    angles = step_ids.astype(jnp.float32)[:, None] * frequency[None, :]
    return jnp.concatenate([jnp.cos(angles), jnp.sin(angles)], axis=1)


def gelu_tanh(value):
    inner = 0.7978845608 * (value + 0.044715 * value * value * value)
    return 0.5 * value * (1.0 + jnp.tanh(inner))


def gelu_slope(value):
    tangent = jnp.tanh(0.7978845608 * (value + 0.044715 * value * value * value))
    return 0.5 * (1.0 + tangent) + 0.5 * value * (1.0 - tangent * tangent) * 0.7978845608 * (
        1.0 + 0.134145 * value * value
    )


def contract_last(left, right):
    return lax.dot_general(
        left, right, (((1,), (1,)), ((), ())), preferred_element_type=jnp.float32
    )


def contract_first(left, right):
    return lax.dot_general(
        left, right, (((0,), (0,)), ((), ())), preferred_element_type=jnp.float32
    )


def forward(tok_rows, step_ids, w_in, w_out, w_time, gain, bias):
    time_feat = jax.nn.silu(sinusoid(step_ids, w_time.shape[0])).astype(jnp.bfloat16)
    embedding = jnp.dot(time_feat, w_time, preferred_element_type=jnp.float32)
    samples = step_ids.shape[0]
    width = tok_rows.shape[1]
    summed = tok_rows.astype(jnp.float32).reshape(samples, -1, width) + embedding[:, None, :]
    summed = summed.reshape(-1, width)
    center = summed - jnp.mean(summed, axis=1, keepdims=True)
    inv_std = lax.rsqrt(jnp.mean(center * center, axis=1, keepdims=True) + 1e-05)
    normed = center * inv_std
    normed_b = (normed * gain + bias).astype(jnp.bfloat16)
    mixed = contract_last(normed_b, w_in)
    hidden_count = w_out.shape[0]
    gate_part = mixed[:, :hidden_count]
    up_part = mixed[:, hidden_count:]
    gelu_gate = gelu_tanh(gate_part)
    hidden = (gelu_gate * up_part).astype(jnp.bfloat16)
    output = summed + jnp.dot(hidden, w_out, preferred_element_type=jnp.float32)
    return (output, (time_feat, normed, inv_std, normed_b, gate_part, up_part, gelu_gate, hidden))


def backward(grad_y, saved, w_in, w_out, gain):
    time_feat, normed, inv_std, normed_b, gate_part, up_part, gelu_gate, hidden = saved
    grad_yb = grad_y.astype(jnp.bfloat16)
    grad_h = contract_last(grad_yb, w_out)
    grad_mix = jnp.concatenate(
        [grad_h * up_part * gelu_slope(gate_part), grad_h * gelu_gate], axis=1
    ).astype(jnp.bfloat16)
    grad_z = jnp.dot(grad_mix, w_in, preferred_element_type=jnp.float32)
    grad_gain = jnp.sum(grad_z * normed, axis=0)
    grad_bias = jnp.sum(grad_z, axis=0)
    grad_n = grad_z * gain
    grad_s = grad_y + inv_std * (
        grad_n
        - jnp.mean(grad_n, axis=1, keepdims=True)
        - normed * jnp.mean(grad_n * normed, axis=1, keepdims=True)
    )
    samples = time_feat.shape[0]
    grad_emb = jnp.sum(grad_s.reshape(samples, -1, grad_s.shape[1]), axis=1)
    grad_time = lax.dot_general(
        time_feat.astype(jnp.float32),
        grad_emb,
        (((0,), (0,)), ((), ())),
        precision=lax.Precision.HIGHEST,
        preferred_element_type=jnp.float32,
    )
    return (grad_yb, grad_mix, grad_gain, grad_bias, grad_time)


def fetch(piece_in, piece_out, piece_time):
    return (
        lax.all_gather(piece_in, "dp", axis=0, tiled=True),
        lax.all_gather(piece_out, "dp", axis=0, tiled=True),
        lax.all_gather(piece_time, "dp", axis=0, tiled=True),
    )


def per_device(
    student_in,
    target_in,
    timesteps,
    student_win,
    student_wout,
    student_wtime,
    student_gain,
    student_bias,
    target_win,
    target_wout,
    target_wtime,
    target_gain,
    target_bias,
):
    s_in, s_out, s_time = fetch(
        student_win.astype(jnp.bfloat16),
        student_wout.astype(jnp.bfloat16),
        student_wtime.astype(jnp.bfloat16),
    )
    student_out, saved = forward(
        student_in, timesteps, s_in, s_out, s_time, student_gain, student_bias
    )
    t_in, t_out, t_time = fetch(
        target_win.astype(jnp.bfloat16),
        target_wout.astype(jnp.bfloat16),
        target_wtime.astype(jnp.bfloat16),
    )
    target_out, unused = forward(
        target_in, timesteps - SKIP, t_in, t_out, t_time, target_gain, target_bias
    )
    grad_y = (student_out - target_out) / student_in.shape[0]
    back_in, back_out = (
        lax.all_gather(student_win.astype(jnp.bfloat16), "dp", axis=0, tiled=True),
        lax.all_gather(student_wout.astype(jnp.bfloat16), "dp", axis=0, tiled=True),
    )
    grad_yb, grad_mix, grad_gain, grad_bias, grad_time = backward(
        grad_y, saved, back_in, back_out, student_gain
    )
    normed_b = saved[3]
    hidden = saved[7]
    part = grad_mix
    shard_in = lax.psum_scatter(
        contract_first(part, normed_b), "dp", scatter_dimension=0, tiled=True
    )
    part = hidden
    shard_out = lax.psum_scatter(
        contract_first(part, grad_yb), "dp", scatter_dimension=0, tiled=True
    )
    shard_time = lax.psum_scatter(grad_time, "dp", scatter_dimension=0, tiled=True)
    shard_in, shard_out, shard_time = lax.psum((shard_in, shard_out, shard_time), "rep")
    total_gain, total_bias = lax.psum((grad_gain, grad_bias), ("dp", "rep"))

    def average(target_p, student_p, grad_p):
        return ema_decay * target_p + (1.0 - ema_decay) * (student_p - learn_rate * grad_p)

    return (
        shard_in,
        shard_out,
        shard_time,
        total_gain,
        total_bias,
        average(target_win, student_win, shard_in),
        average(target_wout, student_wout, shard_out),
        average(target_wtime, student_wtime, shard_time),
        average(target_gain, student_gain, total_gain),
        average(target_bias, student_bias, total_bias),
    )


def time_features(step_ids, width):
    return jax.nn.silu(sinusoid(step_ids, width)).astype(jnp.bfloat16)


def fused_kernel(
    n_rep, n_sam,
    x_s, x_t, tf, sw, so, st, sg, sb, tw, to, tt, tg, tb,
    fin_o, sum_o,
    ws_all, os_all, wt_all, ot_all,
    tf_all, e_part, e_in, small, small_rep,
    normed_v, inv_v, nb_v, hid_v, a_v, b_v, y_v, nbt_v, gyb_v, gma_v, gmb_v,
    g_win, g_out, gb_win, gb_out, r1_win, r1_out, s2_win, s2_out, r2_win, r2_out,
    p_v, pb_v, r3_v, fin_v,
    g_send, g_recv, tf_send, tf_recv, e_send, e_recv, sm_send, sm_recv,
    r1_send, r1_recv, r2_send, r2_recv, r3_send, r3_recv, r4_send, r4_recv, rs_send, rs_recv,
):
    f32, bf16 = jnp.float32, jnp.bfloat16
    me, rep = lax.axis_index("dp"), lax.axis_index("rep")
    core, col, row = lax.rem(me, 2), lax.rem(lax.div(me, 2), 2), lax.div(me, 4)
    rows_in, rows_out, rows_time = sw.shape[0], so.shape[0], st.shape[0]
    tokens, width = x_s.shape[1], x_s.shape[0]
    per = tokens // n_sam
    ff = os_all.shape[0]

    def peer(t):
        flip = lambda b, on: 1 - b if on else b
        return flip(row, t & 4) * 4 + flip(col, t & 2) * 2 + flip(core, t & 1)

    def dp_id(t):
        return {"dp": peer(t)}

    def rep_at(j):
        return lax.rem(rep + j, n_rep)

    sends = []

    def send(src, dst, s_sem, r_sem, where):
        copy = pltpu.make_async_remote_copy(
            src_ref=src, dst_ref=dst, send_sem=s_sem, recv_sem=r_sem,
            device_id=where, device_id_type=MESH,
        )
        copy.start()
        sends.append(copy)

    def arrive(dst, s_sem, r_sem):
        pltpu.make_async_remote_copy(
            src_ref=dst, dst_ref=dst, send_sem=s_sem, recv_sem=r_sem,
            device_id=dp_id(1), device_id_type=MESH,
        ).wait_recv()

    def block(ref, owner, count):
        return ref.at[pl.ds(pl.multiple_of(owner * count, 16), count)]

    bufs = (ws_all, os_all, wt_all, ot_all)
    counts = (rows_in, rows_out, rows_in, rows_out)
    firsts = (2, 4, 4, 2)
    for buf, own, count in zip(bufs, (sw, so, tw, to), counts):
        buf[pl.ds(pl.multiple_of(me * count, 16), count), :] = own[...].astype(bf16)
    tf_all[pl.ds(me, 1)] = tf[pl.ds(me, 1)]

    barrier = pltpu.get_barrier_semaphore()
    for t in range(1, 8):
        pl.semaphore_signal(barrier, inc=1, device_id=dp_id(t), device_id_type=MESH)
    for j in range(1, n_rep):
        pl.semaphore_signal(barrier, inc=1, device_id={"rep": rep_at(j)}, device_id_type=MESH)
    pl.semaphore_wait(barrier, 7 + n_rep - 1)

    def push(seg, orel, t, k):
        part = block(bufs[seg], peer(orel), counts[seg])
        send(part, part, g_send.at[seg * 8 + k], g_recv.at[seg * 8 + (orel ^ t)], dp_id(t))

    def landed(seg, orel):
        arrive(block(bufs[seg], peer(orel), counts[seg]), g_send.at[0], g_recv.at[seg * 8 + orel])

    def open_gather(seg):
        push(seg, 0, firsts[seg], 0)
        push(seg, 0, 6 - firsts[seg], 1)
        push(seg, 0, 1, 2)

    def relay_near(seg):
        first, second = firsts[seg], 6 - firsts[seg]
        landed(seg, first)
        push(seg, first, second, 3)
        push(seg, first, 1, 4)
        landed(seg, second)
        push(seg, second, 1, 5)

    def relay_far(seg):
        landed(seg, 6)
        push(seg, 6, 1, 6)

    def close_gather(seg):
        for orel in (1, 3, 5, 7):
            landed(seg, orel)

    for t in range(1, 8):
        send(tf.at[peer(t)], tf_all.at[me], tf_send.at[t], tf_recv.at[t], dp_id(t))
    open_gather(0)
    for t in range(1, 8):
        arrive(tf_all.at[peer(t)], tf_send.at[t], tf_recv.at[t])
    feats = tf_all[...].reshape(8 * SUB, rows_time).astype(bf16)
    part_s = jnp.dot(feats, st[...].astype(bf16), preferred_element_type=f32)
    part_t = jnp.dot(feats, tt[...].astype(bf16), preferred_element_type=f32)
    line = lax.rem(lax.broadcasted_iota(jnp.int32, part_s.shape, 0), SUB)
    e_part[...] = jnp.where(line < n_sam, part_s, part_t).reshape(e_part.shape)
    e_in[pl.ds(me, 1)] = e_part[pl.ds(me, 1)]
    for t in range(1, 8):
        send(e_part.at[peer(t)], e_in.at[me], e_send.at[t], e_recv.at[t], dp_id(t))
    open_gather(1)
    open_gather(2)
    open_gather(3)
    relay_near(0)
    for t in range(1, 8):
        arrive(e_in.at[peer(t)], e_send.at[t], e_recv.at[t])
    emb = e_in[0]
    for k in range(1, 8):
        emb = emb + e_in[k]

    def normalise(x_ref, k, shift, gain, bias):
        summed = x_ref[:, pl.ds(k * per, per)].astype(f32).T + shift
        center = summed - jnp.mean(summed, axis=1, keepdims=True)
        inv = lax.rsqrt(jnp.mean(center * center, axis=1, keepdims=True) + 1e-05)
        normed = center * inv
        return summed, inv, normed, (normed * gain + bias).astype(bf16)

    for k in range(n_sam):
        at = pl.ds(k * per, per)
        summed, inv, normed, nb = normalise(x_s, k, emb[k : k + 1], sg[...][None], sb[...][None])
        y_v[at, :], normed_v[at, :], nb_v[at, :] = summed, normed, nb
        inv_v[at, :] = inv
    relay_far(0)
    relay_near(1)
    for k in range(n_sam):
        at = pl.ds(k * per, per)
        summed, inv, normed, nb = normalise(x_t, k, emb[n_sam + k : n_sam + k + 1], tg[...][None], tb[...][None])
        y_v[at, :], nbt_v[at, :] = y_v[at, :] - summed, nb
    close_gather(0)
    relay_far(1)

    for k in range(n_sam):
        at = pl.ds(k * per, per)
        gate = contract_last(nb_v[at, :], ws_all[:ff, :])
        up = contract_last(nb_v[at, :], ws_all[ff:, :])
        tangent = jnp.tanh(0.7978845608 * (gate + 0.044715 * gate * gate * gate))
        half = 0.5 * (1.0 + tangent)
        act = gate * half
        slope = half + 0.5 * gate * (1.0 - tangent * tangent) * 0.7978845608 * (
            1.0 + 0.134145 * gate * gate
        )
        a_v[at, :], b_v[at, :] = up * slope, act
        hid_v[at, :] = (act * up).astype(bf16)
        if k == 0:
            relay_near(2)
            close_gather(1)
    relay_far(2)
    relay_near(3)
    for k in range(n_sam):
        at = pl.ds(k * per, per)
        y_v[at, :] = y_v[at, :] + jnp.dot(hid_v[at, :], os_all[...], preferred_element_type=f32)
    close_gather(2)
    relay_far(3)

    for k in range(n_sam):
        at = pl.ds(k * per, per)
        gate = contract_last(nbt_v[at, :], wt_all[:ff, :])
        up = contract_last(nbt_v[at, :], wt_all[ff:, :])
        hid = (gelu_tanh(gate) * up).astype(bf16)
        if k == 0:
            close_gather(3)
        gy = (y_v[at, :] - jnp.dot(hid, ot_all[...], preferred_element_type=f32)) * (1.0 / tokens)
        y_v[at, :], gyb_v[at, :] = gy, gy.astype(bf16)

    total_out = contract_first(hid_v[...], gyb_v[...])
    g_out[...], gb_out[...] = total_out, total_out.astype(bf16)

    def to_core(src, dst, count, q, k):
        send(block(src, 2 * q + 1 - core, count), dst.at[q], r1_send.at[k], r1_recv.at[k], dp_id(1))

    for q in range(4):
        to_core(gb_out, r1_out, rows_out, q, q)

    grad_gain = jnp.zeros((1, width), f32)
    grad_bias = grad_gain
    embs = []
    for k in range(n_sam):
        at = pl.ds(k * per, per)
        gh = contract_last(gyb_v[at, :], os_all[...])
        gma, gmb = (gh * a_v[at, :]).astype(bf16), (gh * b_v[at, :]).astype(bf16)
        gma_v[at, :], gmb_v[at, :] = gma, gmb
        gz = jnp.dot(gma, ws_all[:ff, :], preferred_element_type=f32) + jnp.dot(
            gmb, ws_all[ff:, :], preferred_element_type=f32
        )
        normed = normed_v[at, :]
        grad_gain = grad_gain + jnp.sum(gz * normed, axis=0, keepdims=True)
        grad_bias = grad_bias + jnp.sum(gz, axis=0, keepdims=True)
        gn = gz * sg[...][None]
        gs = y_v[at, :] + inv_v[at, :] * (
            gn
            - jnp.mean(gn, axis=1, keepdims=True)
            - normed * jnp.mean(gn * normed, axis=1, keepdims=True)
        )
        embs.append(jnp.sum(gs, axis=0, keepdims=True))
    fill = jnp.zeros((SUB - n_sam - 2, width), f32)
    small[pl.ds(me, 1)] = jnp.concatenate(embs + [grad_gain, grad_bias, fill], axis=0)[None]

    for h, gm in enumerate((gma_v, gmb_v)):
        total = contract_first(gm[...], nb_v[...])
        at = pl.ds(h * ff, ff)
        g_win[at, :], gb_win[at, :] = total, total.astype(bf16)
        for q in (2 * h, 2 * h + 1):
            to_core(gb_win, r1_win, rows_in, q, 4 + q)
        if h == 0:
            for t in range(1, 8):
                send(small.at[me], small.at[me], sm_send.at[t], sm_recv.at[t], dp_id(t))

    def pair(g, r1, owner_rel, count):
        owner = peer(owner_rel)
        own = g[pl.ds(pl.multiple_of(owner * count, 16), count), :]
        return own + r1[lax.div(owner, 2)].astype(f32)

    for g, r1, s2, r2, count, base in (
        (g_out, r1_out, s2_out, r2_out, rows_out, 0),
        (g_win, r1_win, s2_win, r2_win, rows_in, 4),
    ):
        for q in range(4):
            arrive(r1.at[q], r1_send.at[base + q], r1_recv.at[base + q])
        for k in (3, 1, 2):
            s2[k] = pair(g, r1, 2 * k, count).astype(bf16)
            send(s2.at[k], r2.at[k], r2_send.at[base + k], r2_recv.at[base + k], dp_id(2 * k))

    for t in range(1, 8):
        arrive(small.at[peer(t)], sm_send.at[t], sm_recv.at[t])
    feats = tf_all[...].reshape(8 * SUB, rows_time)
    line = lax.rem(lax.broadcasted_iota(jnp.int32, feats.shape, 0), SUB)
    feats = jnp.where(line < n_sam, feats, 0.0)
    p_v[pl.ds(rows_in + rows_out, rows_time), :] = lax.dot_general(
        feats,
        small[...].reshape(8 * SUB, width),
        (((0,), (0,)), ((), ())),
        precision=lax.Precision.HIGHEST,
        preferred_element_type=f32,
    )
    sums = small[0]
    for k in range(1, 8):
        sums = sums + small[k]
    small_rep[pl.ds(rep, 1)] = sums[None]
    for j in range(1, n_rep):
        send(small_rep.at[rep], small_rep.at[rep], rs_send.at[j], rs_recv.at[j], {"rep": rep_at(j)})

    for g, r1, r2, count, base, start in (
        (g_out, r1_out, r2_out, rows_out, 0, rows_in),
        (g_win, r1_win, r2_win, rows_in, 4, 0),
    ):
        total = pair(g, r1, 0, count)
        for k in (1, 2, 3):
            arrive(r2.at[k], r2_send.at[base + k], r2_recv.at[base + k])
            total = total + r2[k].astype(f32)
        p_v[pl.ds(start, count), :] = total
    pb_v[...] = p_v[...].astype(bf16)

    share = p_v.shape[0] // n_rep
    for j in range(1, n_rep):
        send(block(pb_v, rep_at(j), share), r3_v.at[j], r3_send.at[j], r3_recv.at[j], {"rep": rep_at(j)})
    mine = pl.ds(pl.multiple_of(rep * share, 16), share)
    total = p_v[mine, :]
    for j in range(1, n_rep):
        arrive(r3_v.at[j], r3_send.at[j], r3_recv.at[j])
        total = total + r3_v[j].astype(f32)
    fin_v[mine, :] = total.astype(bf16)
    for j in range(1, n_rep):
        part = block(fin_v, rep, share)
        send(part, part, r4_send.at[j], r4_recv.at[j], {"rep": rep_at(j)})

    for j in range(1, n_rep):
        arrive(small_rep.at[rep_at(n_rep - j)], rs_send.at[j], rs_recv.at[j])
    sums = small_rep[0]
    for j in range(1, n_rep):
        sums = sums + small_rep[j]

    sum_o[...] = sums
    for j in range(1, n_rep):
        arrive(block(fin_v, rep_at(n_rep - j), share), r4_send.at[j], r4_recv.at[j])
    fin_o[...] = fin_v[...]
    for copy in sends:
        copy.wait_send()


def average(target_p, student_p, grad_p):
    return ema_decay * target_p + (1.0 - ema_decay) * (student_p - learn_rate * grad_p)


def update_kernel(
    n_sam, fin, sums, sw, so, st, sg, sb, tw, to, tt, tg, tb,
    gw_o, go_o, gt_o, gg_o, gb_o, ew_o, eo_o, et_o, eg_o, eb_o,
):
    start = 0
    for g_o, e_o, student, target in (
        (gw_o, ew_o, sw, tw), (go_o, eo_o, so, to), (gt_o, et_o, st, tt),
    ):
        grad = fin[pl.ds(start, g_o.shape[0]), :].astype(jnp.float32)
        g_o[...] = grad
        e_o[...] = average(target[...], student[...], grad)
        start += g_o.shape[0]
    gg, gb = sums[n_sam, :], sums[n_sam + 1, :]
    gg_o[...], gb_o[...] = gg, gb
    eg_o[...] = average(tg[...], sg[...], gg)
    eb_o[...] = average(tb[...], sb[...], gb)


def fused_device(n_dp, n_rep, *args):
    (student_in, target_in, timesteps, sw, so, st, sg, sb, tw, to, tt, tg, tb) = args
    f32, bf16 = jnp.float32, jnp.bfloat16
    tokens, width = student_in.shape
    n_sam = timesteps.shape[0]
    rows_in, rows_out, rows_time = sw.shape[0], so.shape[0], st.shape[0]
    ff = rows_out * n_dp
    both = jnp.concatenate([timesteps, timesteps - SKIP])
    feats = time_features(both, rows_time * n_dp).astype(f32)
    feats = jnp.pad(feats, ((0, SUB - 2 * n_sam), (0, 0)))
    feats = feats.reshape(SUB, n_dp, rows_time).transpose(1, 0, 2)
    rows_all = rows_in + rows_out + rows_time
    vm = pltpu.VMEM
    dma = pltpu.SemaphoreType.DMA
    scratch = [
        vm((n_dp * rows_in, width), bf16), vm((ff, width), bf16),
        vm((n_dp * rows_in, width), bf16), vm((ff, width), bf16),
        vm((n_dp, SUB, rows_time), f32), vm((n_dp, SUB, width), f32), vm((n_dp, SUB, width), f32),
        vm((n_dp, SUB, width), f32), vm((n_rep, SUB, width), f32),
        vm((tokens, width), f32), vm((tokens, 1), f32), vm((tokens, width), bf16),
        vm((tokens, ff), bf16), vm((tokens, ff), f32), vm((tokens, ff), f32),
        vm((tokens, width), f32), vm((tokens, width), bf16), vm((tokens, width), bf16),
        vm((tokens, ff), bf16), vm((tokens, ff), bf16),
        vm((n_dp * rows_in, width), f32), vm((ff, width), f32),
        vm((n_dp * rows_in, width), bf16), vm((ff, width), bf16),
        vm((4, rows_in, width), bf16), vm((4, rows_out, width), bf16),
        vm((4, rows_in, width), bf16), vm((4, rows_out, width), bf16),
        vm((4, rows_in, width), bf16), vm((4, rows_out, width), bf16),
        vm((rows_all, width), f32), vm((rows_all, width), bf16),
        vm((n_rep, rows_all // n_rep, width), bf16), vm((rows_all, width), bf16),
        dma((32,)), dma((32,)), dma((8,)), dma((8,)), dma((8,)), dma((8,)), dma((8,)), dma((8,)),
        dma((8,)), dma((8,)), dma((8,)), dma((8,)),
        dma((n_rep,)), dma((n_rep,)), dma((n_rep,)), dma((n_rep,)), dma((n_rep,)), dma((n_rep,)),
    ]
    big = [jax.ShapeDtypeStruct(w.shape, f32) for w in (sw, so, st)]
    flat = [jax.ShapeDtypeStruct((width,), f32)] * 2
    fin, sums = pl.pallas_call(
        functools.partial(fused_kernel, n_rep, n_sam),
        out_shape=(
            jax.ShapeDtypeStruct((rows_all, width), bf16),
            jax.ShapeDtypeStruct((SUB, width), f32),
        ),
        in_specs=[pl.BlockSpec(memory_space=vm)] * 13,
        out_specs=[pl.BlockSpec(memory_space=vm)] * 2,
        scratch_shapes=scratch,
        compiler_params=pltpu.CompilerParams(
            collective_id=0, has_side_effects=True, vmem_limit_bytes=56 * 1024 * 1024
        ),
        name="distill_step",
    )(student_in.T, target_in.T, feats, sw, so, st, sg, sb, tw, to, tt, tg, tb)
    return tuple(
        pl.pallas_call(
            functools.partial(update_kernel, n_sam),
            out_shape=(*big, *flat, *big, *flat),
            in_specs=[pl.BlockSpec(memory_space=vm)] * 12,
            out_specs=[pl.BlockSpec(memory_space=vm)] * 10,
            name="average_step",
        )(fin, sums, sw, so, st, sg, sb, tw, to, tt, tg, tb)
    )


def fits_fused(n_dp, n_rep, args):
    tokens, samples = args[0].shape[0], args[2].shape[0]
    n_dev = n_dp * n_rep
    rows = [args[i].shape[0] for i in (3, 4, 5)]
    return (
        n_dp == 8
        and n_rep > 1
        and samples % n_dev == 0
        and 2 * (samples // n_dev) + 0 <= SUB
        and samples // n_dev + 2 <= SUB
        and tokens % samples == 0
        and (tokens // samples) % 128 == 0
        and all(r % (16 * n_dp) == 0 for r in rows)
        and (sum(rows) // n_dp) % (16 * n_rep) == 0
        and rows[0] == 2 * rows[1]
    )


def solution(mesh):
    in_specs = (
        P(("dp", "rep"), None),
        P(("dp", "rep"), None),
        P(("dp", "rep")),
        P("dp", None),
        P("dp", None),
        P("dp", None),
        P(),
        P(),
        P("dp", None),
        P("dp", None),
        P("dp", None),
        P(),
        P(),
    )
    out_specs = (
        P("dp", None),
        P("dp", None),
        P("dp", None),
        P(),
        P(),
        P("dp", None),
        P("dp", None),
        P("dp", None),
        P(),
        P(),
    )
    n_dp, n_rep = mesh.shape["dp"], mesh.shape["rep"]

    def step(*args):
        fused = fits_fused(n_dp, n_rep, args)
        body = functools.partial(fused_device, n_dp, n_rep) if fused else per_device
        return jax.shard_map(
            body, mesh=mesh, in_specs=in_specs, out_specs=out_specs, check_vma=False
        )(*args)

    return step
```
